32 devices in a mesh: grp: 8 (over y, x, core), shard: 4 (over z).
Axes of the slice: x: 2, y: 2, z: 4, core: 2. Of those that a mesh axis runs over, the one named last changes fastest.
Arguments:
- gradients: bfloat16 [8, 1024, 5120], P('grp', None, 'shard'), may hold values from -150 to 150
- left_factor: bfloat16 [8, 1024, 1024], P('grp'), may hold values from -1 to 2, as said below
- right_factor: bfloat16 [8, 5120, 5120], P('grp', 'shard'), may hold values from -1 to 2, as said below
Outputs:
- update: bfloat16 [8, 1024, 5120], P('grp', None, 'shard')
The draws below stay inside these ranges and needn't reach their ends.
Inputs may be any that keep to these rules, and one draw needn't show every extreme that they name: `left_factor`: each factor is upper triangular with a positive diagonal. `right_factor`: each factor is upper triangular with a positive diagonal.
All inputs are finite; a program needn't handle non-finite values.
Results may differ from the reference program's by a relative error of at most 0.0061.
Values may be sent and summed in bfloat16 or wider, within the bound.
A program may use at most 128 MiB of HBM per device.

```python
import math
import jax
import jax.numpy as jnp
from jax import lax

D = 5120
KV_WIDTH = 1024
WEIGHTS = 8


def triangular(key, count, width):
    keys = jax.random.split(jax.random.fold_in(key, 7), 2)
    diagonal = jax.random.uniform(keys[0], (count, width), minval=0.6, maxval=1.4)
    offdiag = jnp.clip(jax.random.normal(keys[1], (count, width, width)), -3.0, 3.0) * (0.7 / math.sqrt(width))
    upper = jnp.triu(offdiag, 1)
    return upper + diagonal[:, :, None] * jnp.eye(width, dtype=jnp.float32)[None]


def draw_left_factor(key, part):
    return triangular(jax.random.fold_in(key, 11), WEIGHTS, KV_WIDTH).astype(jnp.bfloat16)


def draw_right_factor(key, part):
    return triangular(jax.random.fold_in(key, 13), WEIGHTS, D).astype(jnp.bfloat16)


def draw_gradients(key, part):
    keys = jax.random.split(jax.random.fold_in(key, 17), 4)
    top = math.log(math.sqrt(10.0))
    row_scale = jnp.exp(jax.random.uniform(keys[0], (WEIGHTS, KV_WIDTH), minval=0.0, maxval=top))
    col_scale = jnp.exp(jax.random.uniform(keys[1], (WEIGHTS, D), minval=0.0, maxval=top))
    weight_scale = jnp.exp(jax.random.uniform(keys[2], (WEIGHTS,), minval=0.0, maxval=math.log(3.0)))
    base = jnp.clip(jax.random.normal(keys[3], (WEIGHTS, KV_WIDTH, D)), -5.0, 5.0)
    values = base * row_scale[:, :, None] * col_scale[:, None, :] * weight_scale[:, None, None]
    return values.astype(jnp.bfloat16)


def setup_inputs(seed: int = 0) -> dict:
    arg_keys = jax.random.split(jax.random.key(seed), 4)
    gradients = draw_gradients(jax.random.fold_in(arg_keys[3], 71), 0)
    left_factor = draw_left_factor(jax.random.fold_in(arg_keys[3], 71), 0)
    right_factor = draw_right_factor(jax.random.fold_in(arg_keys[3], 71), 0)
    return dict(gradients=gradients, left_factor=left_factor, right_factor=right_factor)


def precondition(items):
    gradient, left_q, right_q = items
    first = lax.dot_general(gradient, right_q, (((1,), (1,)), ((), ())), preferred_element_type=jnp.float32).astype(jnp.bfloat16)
    second = jnp.dot(first, right_q, preferred_element_type=jnp.float32).astype(jnp.bfloat16)
    third = jnp.dot(left_q, second, preferred_element_type=jnp.float32).astype(jnp.bfloat16)
    return lax.dot_general(left_q, third, (((0,), (0,)), ((), ())), preferred_element_type=jnp.float32)

def reference(gradients, left_factor, right_factor):
    precond = lax.map(precondition, (gradients, left_factor, right_factor))
    count = precond.shape[0] * precond.shape[1] * precond.shape[2]
    rms = jnp.sqrt(jnp.sum(precond * precond) / count + 1e-06)
    factor = jnp.minimum(jnp.float32(1.0), 1.1 / rms)
    return (precond * factor).astype(jnp.bfloat16)
```

```python
import functools

import jax
import jax.numpy as jnp
from jax import lax
from jax.experimental import pallas as pl
from jax.experimental.pallas import tpu as pltpu
from jax.sharding import PartitionSpec as P

MESH = pl.DeviceIdType.MESH
VMEM_BYTES = 67_000_000
AHEAD = 2


def plain_body(gradients, left_factor, right_factor):
    gradient = gradients[0]
    left_q = left_factor[0]
    block = right_factor[0]
    first = lax.dot_general(
        lax.all_gather(gradient, "shard", axis=1, tiled=True),
        block,
        (((1,), (1,)), ((), ())),
        preferred_element_type=jnp.float32,
    ).astype(jnp.bfloat16)
    second_rows = lax.psum_scatter(
        lax.dot_general(block, first, (((0,), (1,)), ((), ())), preferred_element_type=jnp.float32),
        "shard",
        scatter_dimension=0,
        tiled=True,
    ).astype(jnp.bfloat16)
    second = second_rows.T
    third = jnp.dot(left_q, second, preferred_element_type=jnp.float32).astype(jnp.bfloat16)
    precond = lax.dot_general(
        left_q, third, (((0,), (0,)), ((), ())), preferred_element_type=jnp.float32
    )
    total = lax.psum(jnp.sum(precond * precond), ("grp", "shard"))
    count = precond.size * lax.axis_size("grp") * lax.axis_size("shard")
    rms = jnp.sqrt(total / count + 1e-06)
    factor = jnp.minimum(jnp.float32(1.0), 1.1 / rms)
    return (precond * factor).astype(jnp.bfloat16)[None]


def kernel(
    n, groups, m, g_hbm, q_hbm, r_hbm, out_hbm, factor_ref,
    gbuf, rbuf, qbuf, psend, precv, second, precond, acc, fst, thr, sq, sq_recv,
    load_sem, gsend, grecv, psend_sem, precv_sem, sq_send_sem, sq_recv_sem, out_sem,
):
    s = lax.axis_index("shard")
    g = lax.axis_index("grp")
    height, width = g_hbm.shape
    chunks = height // m
    lower = lax.rem(s + n - 1, n)
    upper = lax.rem(s + 1, n)

    def rows(t):
        return pl.ds(pl.multiple_of((chunks - 1 - t) * m, m), m)

    def load_r(d):
        cols = pl.ds(pl.multiple_of((s + d) * width, 128), width)
        return pltpu.make_async_copy(r_hbm.at[:, cols], rbuf.at[d], load_sem.at[d])

    load_g = pltpu.make_async_copy(g_hbm, gbuf.at[0], load_sem.at[n])
    load_q = pltpu.make_async_copy(q_hbm, qbuf, load_sem.at[n + 1])
    load_g.start()
    for d in range(n):
        pl.when(s + d < n)(lambda d=d: load_r(d).start())
    load_q.start()

    barrier = pltpu.get_barrier_semaphore()
    for o in range(1, n):
        pl.semaphore_signal(barrier, inc=1, device_id={"shard": lax.rem(s + o, n)}, device_id_type=MESH)
    for o in range(1, groups):
        pl.semaphore_signal(barrier, inc=1, device_id={"grp": lax.rem(g + o, groups)}, device_id_type=MESH)
    pl.semaphore_wait(barrier, n - 1 + groups - 1)

    def g_copy(t, k):
        src = g_hbm.at[rows(t)] if k == 1 else gbuf.at[k - 1, rows(t)]
        return pltpu.make_async_remote_copy(
            src_ref=src, dst_ref=gbuf.at[k, rows(t)],
            send_sem=gsend.at[t, k - 1], recv_sem=grecv.at[t, k - 1],
            device_id={"shard": lower}, device_id_type=MESH,
        )

    def p_copy(t, d):
        return pltpu.make_async_remote_copy(
            src_ref=psend.at[d - 1, rows(t)], dst_ref=precv.at[d - 1, rows(t)],
            send_sem=psend_sem.at[t, d - 1], recv_sem=precv_sem.at[t, d - 1],
            device_id={"shard": upper}, device_id_type=MESH,
        )

    def forward(t):
        @pl.when(s >= 1)
        def _():
            g_copy(t, 1).start()
            for k in range(2, n):
                @pl.when(s + k - 1 < n)
                def _(k=k):
                    g_copy(t, k - 1).wait_recv()
                    g_copy(t, k).start()

    forward(0)
    second[...] = jnp.zeros_like(second)
    precond[...] = jnp.zeros_like(precond)
    for t in range(1, min(AHEAD, chunks)):
        forward(t)
    load_g.wait()
    for d in range(n):
        pl.when(s + d < n)(lambda d=d: load_r(d).wait())
    load_q.wait()

    def step(t, carry):
        pl.when(t + AHEAD < chunks)(lambda: forward(t + AHEAD))
        here = rows(t)
        acc[...] = jnp.zeros_like(acc)

        def first_part(d, carry):
            for k in range(1, n):
                pl.when((s == 0) & (d == k))(lambda k=k: g_copy(t, k).wait_recv())
            acc[...] += lax.dot_general(
                gbuf[d, here, :], rbuf[d], (((1,), (1,)), ((), ())),
                preferred_element_type=jnp.float32,
            )
            return carry

        lax.fori_loop(0, n - s, first_part, 0)
        fst[...] = acc[...].astype(fst.dtype)

        def second_part(i, carry):
            d = n - 1 - s - i
            acc[...] = jnp.dot(fst[...], rbuf[d], preferred_element_type=jnp.float32)

            @pl.when(s >= 1)
            def _():
                p_copy(t, d + 1).wait_recv()
                acc[...] += precv[d, here, :].astype(jnp.float32)

            @pl.when(d >= 1)
            def _():
                psend[d - 1, here, :] = acc[...].astype(psend.dtype)
                p_copy(t, d).start()

            @pl.when(d == 0)
            def _():
                second[here, :] = acc[...].astype(second.dtype)

            return carry

        lax.fori_loop(0, n - s, second_part, 0)

        tile = 256 if width % 256 == 0 else 128

        def left_part(i, carry):
            cols = pl.ds(pl.multiple_of(i * tile, tile), tile)
            third = jnp.dot(
                qbuf[here, :], second[:, cols], preferred_element_type=jnp.float32
            ).astype(jnp.bfloat16)
            precond[:, cols] += lax.dot_general(
                qbuf[here, :], third, (((0,), (0,)), ((), ())),
                preferred_element_type=jnp.float32,
            )
            return carry

        lax.fori_loop(0, width // tile, left_part, 0)
        return carry

    lax.fori_loop(0, chunks, step, 0)

    write = pltpu.make_async_copy(precond, out_hbm, out_sem)
    write.start()

    thr[...] = jnp.zeros_like(thr)

    def square(i, carry):
        part = precond[pl.ds(pl.multiple_of(i * m, m), m), :]
        thr[...] += jnp.sum((part * part).reshape(m // 8, 8, width), axis=0)
        return carry

    lax.fori_loop(0, chunks, square, 0)
    mine = thr[:, :128]
    for c in range(1, width // 128):
        mine += thr[:, c * 128:(c + 1) * 128]

    def exchange(stage, value, axis, index, size, base):
        sq[stage] = value
        copies = [
            pltpu.make_async_remote_copy(
                src_ref=sq.at[stage], dst_ref=sq_recv.at[base + o - 1],
                send_sem=sq_send_sem.at[base + o - 1], recv_sem=sq_recv_sem.at[base + o - 1],
                device_id={axis: lax.rem(index + o, size)}, device_id_type=MESH,
            )
            for o in range(1, size)
        ]
        for copy in copies:
            copy.start()
        for copy in copies:
            copy.wait()
        for o in range(1, size):
            value += sq_recv[base + o - 1]
        return value

    value = exchange(0, mine, "shard", s, n, 0)
    value = exchange(1, value, "grp", g, groups, n - 1)
    total = jnp.sum(value)
    count = height * width * n * groups
    rms = jnp.sqrt(jnp.full((8, 128), total) / count + 1e-06)
    factor_ref[...] = jnp.minimum(jnp.float32(1.0), 1.1 / rms)

    def drain(t, carry):
        for k in range(1, n):
            pl.when((s >= 1) & (s + k - 1 < n))(lambda k=k: g_copy(t, k).wait_send())
            pl.when(s + k < n)(lambda k=k: p_copy(t, k).wait_send())
        return carry

    lax.fori_loop(0, chunks, drain, 0)
    write.wait()


def fused_body(n, groups, m, gradients, left_factor, right_factor):
    height, width = gradients.shape[1:]
    chunks = height // m
    bf16, f32 = jnp.bfloat16, jnp.float32
    dma = pltpu.SemaphoreType.DMA
    peers = n - 1 + groups - 1
    precond, factor = pl.pallas_call(
        functools.partial(kernel, n, groups, m),
        out_shape=(
            jax.ShapeDtypeStruct((height, width), f32),
            jax.ShapeDtypeStruct((8, 128), f32),
        ),
        in_specs=[pl.BlockSpec(memory_space=pl.ANY)] * 3,
        out_specs=(
            pl.BlockSpec(memory_space=pl.ANY),
            pl.BlockSpec(memory_space=pltpu.VMEM),
        ),
        scratch_shapes=[
            pltpu.VMEM((n, height, width), bf16),
            pltpu.VMEM((n, width, width), bf16),
            pltpu.VMEM((height, height), bf16),
            pltpu.VMEM((n - 1, height, width), bf16),
            pltpu.VMEM((n - 1, height, width), bf16),
            pltpu.VMEM((height, width), bf16),
            pltpu.VMEM((height, width), f32),
            pltpu.VMEM((m, width), f32),
            pltpu.VMEM((m, width), bf16),
            pltpu.VMEM((8, width), f32),
            pltpu.VMEM((2, 8, 128), f32),
            pltpu.VMEM((peers, 8, 128), f32),
            dma((n + 2,)),
            dma((chunks, n - 1)),
            dma((chunks, n - 1)),
            dma((chunks, n - 1)),
            dma((chunks, n - 1)),
            dma((peers,)),
            dma((peers,)),
            dma,
        ],
        compiler_params=pltpu.CompilerParams(
            collective_id=0, has_side_effects=True, vmem_limit_bytes=VMEM_BYTES
        ),
        name="kron_precondition",
    )(gradients[0], left_factor[0], right_factor[0])
    return (precond * factor[0, 0]).astype(jnp.bfloat16)[None]


def solution(mesh):
    n, groups = mesh.shape["shard"], mesh.shape["grp"]
    m = 128

    def body(gradients, left_factor, right_factor):
        height, width = gradients.shape[1:]
        need = 2 * (n * width * width + height * height + (3 * n + 1) * height * width)
        fits = need < VMEM_BYTES - 8_000_000
        if gradients.shape[0] == 1 and n > 1 and groups > 1 and width % 128 == 0 and height % m == 0 and fits:
            return fused_body(n, groups, m, gradients, left_factor, right_factor)
        return plain_body(gradients, left_factor, right_factor)

    in_specs = (P("grp", None, "shard"), P("grp", None, None), P("grp", "shard", None))
    out_specs = P("grp", None, "shard")
    return jax.shard_map(body, mesh=mesh, in_specs=in_specs, out_specs=out_specs, check_vma=False)
```

```python
import functools

import jax
import jax.numpy as jnp
from jax import lax
from jax.experimental import pallas as pl
from jax.experimental.pallas import tpu as pltpu
from jax.sharding import PartitionSpec as P

MESH = pl.DeviceIdType.MESH
VMEM_BYTES = 67_000_000
CHUNK_ROWS = 64
AHEAD_PER_SHARD = 3


def plain_body(gradients, left_factor, right_factor):
    gradient = gradients[0]
    left_q = left_factor[0]
    block = right_factor[0]
    first = lax.dot_general(
        lax.all_gather(gradient, "shard", axis=1, tiled=True),
        block,
        (((1,), (1,)), ((), ())),
        preferred_element_type=jnp.float32,
    ).astype(jnp.bfloat16)
    second_rows = lax.psum_scatter(
        lax.dot_general(block, first, (((0,), (1,)), ((), ())), preferred_element_type=jnp.float32),
        "shard",
        scatter_dimension=0,
        tiled=True,
    ).astype(jnp.bfloat16)
    second = second_rows.T
    third = jnp.dot(left_q, second, preferred_element_type=jnp.float32).astype(jnp.bfloat16)
    precond = lax.dot_general(
        left_q, third, (((0,), (0,)), ((), ())), preferred_element_type=jnp.float32
    )
    total = lax.psum(jnp.sum(precond * precond), ("grp", "shard"))
    count = precond.size * lax.axis_size("grp") * lax.axis_size("shard")
    rms = jnp.sqrt(total / count + 1e-06)
    factor = jnp.minimum(jnp.float32(1.0), 1.1 / rms)
    return (precond * factor).astype(jnp.bfloat16)[None]


def kernel(
    n, groups, m, g_hbm, q_hbm, r_hbm, out_hbm, factor_ref,
    gbuf, rbuf, qbuf, psend, precv, second, precond, acc, fst, thr, sq, sq_recv,
    load_sem, gsend, grecv, psend_sem, precv_sem, sq_send_sem, sq_recv_sem, out_sem,
):
    s = lax.axis_index("shard")
    g = lax.axis_index("grp")
    height, width = g_hbm.shape
    chunks = height // m
    lower = lax.rem(s + n - 1, n)
    upper = lax.rem(s + 1, n)

    def rows(t):
        return pl.ds(pl.multiple_of((chunks - 1 - t) * m, m), m)

    def load_r(d):
        cols = pl.ds(pl.multiple_of((s + d) * width, 128), width)
        return pltpu.make_async_copy(r_hbm.at[:, cols], rbuf.at[d], load_sem.at[d])

    load_g = pltpu.make_async_copy(g_hbm, gbuf.at[0], load_sem.at[n])
    load_q = pltpu.make_async_copy(q_hbm, qbuf, load_sem.at[n + 1])
    load_g.start()
    for d in range(n):
        pl.when(s + d < n)(lambda d=d: load_r(d).start())
    load_q.start()

    barrier = pltpu.get_barrier_semaphore()
    for o in range(1, n):
        pl.semaphore_signal(barrier, inc=1, device_id={"shard": lax.rem(s + o, n)}, device_id_type=MESH)
    for o in range(1, groups):
        pl.semaphore_signal(barrier, inc=1, device_id={"grp": lax.rem(g + o, groups)}, device_id_type=MESH)
    pl.semaphore_wait(barrier, n - 1 + groups - 1)

    def g_copy(t, k):
        src = g_hbm.at[rows(t)] if k == 1 else gbuf.at[k - 1, rows(t)]
        return pltpu.make_async_remote_copy(
            src_ref=src, dst_ref=gbuf.at[k, rows(t)],
            send_sem=gsend.at[t, k - 1], recv_sem=grecv.at[t, k - 1],
            device_id={"shard": lower}, device_id_type=MESH,
        )

    def p_copy(t, d):
        return pltpu.make_async_remote_copy(
            src_ref=psend.at[d - 1, rows(t)], dst_ref=precv.at[d - 1, rows(t)],
            send_sem=psend_sem.at[t, d - 1], recv_sem=precv_sem.at[t, d - 1],
            device_id={"shard": upper}, device_id_type=MESH,
        )

    def forward(t):
        @pl.when(s >= 1)
        def _():
            g_copy(t, 1).start()
            for k in range(2, n):
                @pl.when(s + k - 1 < n)
                def _(k=k):
                    g_copy(t, k - 1).wait_recv()
                    g_copy(t, k).start()

    ahead = jnp.where(s == n - 1, chunks, jnp.minimum(AHEAD_PER_SHARD * s, chunks))
    pl.when(ahead >= 1)(lambda: forward(0))
    second[...] = jnp.zeros_like(second)
    precond[...] = jnp.zeros_like(precond)

    def early(t, carry):
        forward(t)
        return carry

    lax.fori_loop(1, ahead, early, 0)
    load_g.wait()
    for d in range(n):
        pl.when(s + d < n)(lambda d=d: load_r(d).wait())
    load_q.wait()

    def step(t, carry):
        pl.when(t + ahead < chunks)(lambda: forward(t + ahead))
        here = rows(t)
        acc[...] = jnp.zeros_like(acc)

        def first_part(d, carry):
            for k in range(1, n):
                pl.when((s == 0) & (d == k))(lambda k=k: g_copy(t, k).wait_recv())
            acc[...] += lax.dot_general(
                gbuf[d, here, :], rbuf[d], (((1,), (1,)), ((), ())),
                preferred_element_type=jnp.float32,
            )
            return carry

        lax.fori_loop(0, n - s, first_part, 0)
        fst[...] = acc[...].astype(fst.dtype)

        def second_part(i, carry):
            d = n - 1 - s - i
            acc[...] = jnp.dot(fst[...], rbuf[d], preferred_element_type=jnp.float32)

            @pl.when(s >= 1)
            def _():
                p_copy(t, d + 1).wait_recv()
                acc[...] += precv[d, here, :].astype(jnp.float32)

            @pl.when(d >= 1)
            def _():
                psend[d - 1, here, :] = acc[...].astype(psend.dtype)
                p_copy(t, d).start()

            @pl.when(d == 0)
            def _():
                second[here, :] = acc[...].astype(second.dtype)

            return carry

        lax.fori_loop(0, n - s, second_part, 0)

        tile = width // 2 if width % 256 == 0 else 128

        def left_part(i, carry):
            cols = pl.ds(pl.multiple_of(i * tile, tile), tile)
            third = jnp.dot(
                qbuf[here, :], second[:, cols], preferred_element_type=jnp.float32
            ).astype(jnp.bfloat16)
            precond[:, cols] += lax.dot_general(
                qbuf[here, :], third, (((0,), (0,)), ((), ())),
                preferred_element_type=jnp.float32,
            )
            return carry

        lax.fori_loop(0, width // tile, left_part, 0)
        return carry

    lax.fori_loop(0, chunks, step, 0)

    write = pltpu.make_async_copy(precond, out_hbm, out_sem)
    write.start()

    thr[...] = jnp.zeros_like(thr)

    def square(i, carry):
        part = precond[pl.ds(pl.multiple_of(i * m, m), m), :]
        thr[...] += jnp.sum((part * part).reshape(m // 8, 8, width), axis=0)
        return carry

    lax.fori_loop(0, chunks, square, 0)
    mine = thr[:, :128]
    for c in range(1, width // 128):
        mine += thr[:, c * 128:(c + 1) * 128]

    def exchange(stage, value, axis, index, size, base):
        sq[stage] = value
        copies = [
            pltpu.make_async_remote_copy(
                src_ref=sq.at[stage], dst_ref=sq_recv.at[base + o - 1],
                send_sem=sq_send_sem.at[base + o - 1], recv_sem=sq_recv_sem.at[base + o - 1],
                device_id={axis: lax.rem(index + o, size)}, device_id_type=MESH,
            )
            for o in range(1, size)
        ]
        for copy in copies:
            copy.start()
        for copy in copies:
            copy.wait()
        for o in range(1, size):
            value += sq_recv[base + o - 1]
        return value

    value = exchange(0, mine, "shard", s, n, 0)
    value = exchange(1, value, "grp", g, groups, n - 1)
    total = jnp.sum(value)
    count = height * width * n * groups
    rms = jnp.sqrt(jnp.full((8, 128), total) / count + 1e-06)
    factor_ref[...] = jnp.minimum(jnp.float32(1.0), 1.1 / rms)

    def drain(t, carry):
        for k in range(1, n):
            pl.when((s >= 1) & (s + k - 1 < n))(lambda k=k: g_copy(t, k).wait_send())
            pl.when(s + k < n)(lambda k=k: p_copy(t, k).wait_send())
        return carry

    lax.fori_loop(0, chunks, drain, 0)
    write.wait()


def fused_body(n, groups, m, gradients, left_factor, right_factor):
    height, width = gradients.shape[1:]
    chunks = height // m
    bf16, f32 = jnp.bfloat16, jnp.float32
    dma = pltpu.SemaphoreType.DMA
    peers = n - 1 + groups - 1
    precond, factor = pl.pallas_call(
        functools.partial(kernel, n, groups, m),
        out_shape=(
            jax.ShapeDtypeStruct((height, width), f32),
            jax.ShapeDtypeStruct((8, 128), f32),
        ),
        in_specs=[pl.BlockSpec(memory_space=pl.ANY)] * 3,
        out_specs=(
            pl.BlockSpec(memory_space=pl.ANY),
            pl.BlockSpec(memory_space=pltpu.VMEM),
        ),
        scratch_shapes=[
            pltpu.VMEM((n, height, width), bf16),
            pltpu.VMEM((n, width, width), bf16),
            pltpu.VMEM((height, height), bf16),
            pltpu.VMEM((n - 1, height, width), bf16),
            pltpu.VMEM((n - 1, height, width), bf16),
            pltpu.VMEM((height, width), bf16),
            pltpu.VMEM((height, width), f32),
            pltpu.VMEM((m, width), f32),
            pltpu.VMEM((m, width), bf16),
            pltpu.VMEM((8, width), f32),
            pltpu.VMEM((2, 8, 128), f32),
            pltpu.VMEM((peers, 8, 128), f32),
            dma((n + 2,)),
            dma((chunks, n - 1)),
            dma((chunks, n - 1)),
            dma((chunks, n - 1)),
            dma((chunks, n - 1)),
            dma((peers,)),
            dma((peers,)),
            dma,
        ],
        compiler_params=pltpu.CompilerParams(
            collective_id=0, has_side_effects=True, vmem_limit_bytes=VMEM_BYTES
        ),
        name="kron_precondition",
    )(gradients[0], left_factor[0], right_factor[0])
    return (precond * factor[0, 0]).astype(jnp.bfloat16)[None]


def solution(mesh):
    n, groups = mesh.shape["shard"], mesh.shape["grp"]
    m = CHUNK_ROWS

    def body(gradients, left_factor, right_factor):
        height, width = gradients.shape[1:]
        need = 2 * (n * width * width + height * height + (3 * n + 1) * height * width)
        fits = need < VMEM_BYTES - 8_000_000
        if gradients.shape[0] == 1 and n > 1 and groups > 1 and width % 128 == 0 and height % m == 0 and fits:
            return fused_body(n, groups, m, gradients, left_factor, right_factor)
        return plain_body(gradients, left_factor, right_factor)

    in_specs = (P("grp", None, "shard"), P("grp", None, None), P("grp", "shard", None))
    out_specs = P("grp", None, "shard")
    return jax.shard_map(body, mesh=mesh, in_specs=in_specs, out_specs=out_specs, check_vma=False)
```
